512 devices in a mesh: grp: 2 (over y), smp: 32 (over z), blk: 4 (over x), pen: 2 (over core).
Axes of the slice: x: 4, y: 2, z: 32, core: 2. Of those that a mesh axis runs over, the one named last changes fastest.
The devices are a block of a 4x8x32 slice.
Arguments:
- allele_matrix: bfloat16 [16384, 8192], P('smp', ('grp', 'blk')), parts along dimension 1, may hold values from -6 to 6
- orthonormal_frames: bfloat16 [16, 512, 512], P(('grp', 'blk')), parts along dimension 0, may hold values from -0.25 to 0.25
- segment_variances: float32 [16, 512], P(('grp', 'blk')), parts along dimension 0, may hold values from 163.84 to 16384
- lambda_grid: float32 [4], replicated, may hold values from 163.84 to 16384
- trait_levels: bfloat16 [16384, 256], P('smp', ('grp', 'pen')), parts along dimension 1, may hold values from -6 to 6
- partition_labels: int32 [16384], P('smp'), may hold values from 0 to 3
- preceding_fits: bfloat16 [4, 16384, 1536], P(('grp', 'pen'), 'smp', 'blk'), parts along dimension 0, may hold values from -6 to 6
Outputs:
- level0_predictions: bfloat16 [16384, 16, 4, 128], P('smp', ('grp', 'blk'), None, 'pen'), parts along dimension 1
- gram_old: float32 [4, 1536, 1536], P(('grp', 'pen'), 'blk', 'smp'), parts along dimension 0
- gram_cross: float32 [4, 32, 1536], P(('grp', 'pen'), 'blk', 'smp'), parts along dimension 0
- gram_new: float32 [4, 32, 32], P(('grp', 'pen'), 'blk'), parts along dimension 0
- fit_old: float32 [4, 1536], P(('grp', 'pen'), 'smp'), parts along dimension 0
- fit_new: float32 [4, 32], P(('grp', 'pen'), 'blk'), parts along dimension 0
The draws below stay inside these ranges and needn't reach their ends.
There are 2 independent parts, one for each index of `grp`. The reference program is written for one: setup_inputs(seed, part) draws one part's arguments, and reference() takes and returns one part's arrays. A program takes and returns all parts, laid end to end along the dimension named above; an argument that names none is the same for every part. Nothing has to cross between parts.
All inputs are finite; a program needn't handle non-finite values.
Results may differ from the reference program's by a relative error of at most 0.018.
Values may be sent and summed in bfloat16 or wider, within the bound.
No kernel may reach another device: no remote copies, remote signals or barrier semaphores. Data moves between devices by JAX's collectives and lax.ppermute only.
A program may use at most 64 MiB of HBM per device.

```python
import math
import jax
import jax.numpy as jnp
from jax import lax

VARIANT_COUNT = 512
PROTEIN_COUNT = 128
LAMBDA_GRID_SIZE = 4
FOLDS = 4
EARLIER = 1536
SAMPLE_TOTAL = 16384
BLOCK_TOTAL = 8


def plant(result, stream_key, smallest, largest):
    longest = result.shape.index(max(result.shape))
    spots = []
    for shift in (0, 1):
        where = [jax.random.randint(jax.random.fold_in(stream_key, axis), (), 0, length) for axis, length in enumerate(result.shape)]
        where[longest] = (where[longest] + shift) % result.shape[longest]
        spots.append(tuple(where))
    return result.at[spots[0]].set(smallest).at[spots[1]].set(largest)


def block_scale(key, shape, shards, smallest, top_value):
    def one(position, shards_of):
        draws = jax.random.uniform(jax.random.fold_in(jax.random.fold_in(key, 6), position), (shards_of,), jnp.float32, smallest / len(shards), top_value / len(shards))
        return jnp.repeat(jnp.exp(draws), shape[position] // shards_of).reshape((-1,) + (1,) * (len(shape) - position - 1))

    loudness = one(*shards[0])
    for cut in shards[1:]:
        loudness = loudness * one(*cut)
    return loudness


def gaussian(key, dims, deviation, reach, shards=(), held_as=jnp.bfloat16):
    level = block_scale(key, dims, shards, -0.22, 0.18) if shards else 1.0
    array = jax.random.normal(key, dims, jnp.float32) * deviation * level
    return jnp.minimum(jnp.maximum(array, -reach), reach).astype(held_as)


def setup_inputs(seed: int = 0, part: int = 0) -> dict:
    arg_keys = jax.random.split(jax.random.key(seed), 8)
    part_splits = jax.random.split(jax.random.fold_in(arg_keys[7], part), 8)
    allele_matrix = gaussian(part_splits[0], (SAMPLE_TOTAL, BLOCK_TOTAL * VARIANT_COUNT), 1.0, 6.0, ((0, 32), (1, 4)))
    orthonormal_frames = gaussian(part_splits[1], (BLOCK_TOTAL, VARIANT_COUNT, VARIANT_COUNT), VARIANT_COUNT ** -0.5, 0.25, ((0, 4),))
    segment_variances = jnp.clip(jnp.exp(math.log(16384.0) - 4.6051702 * jax.random.uniform(part_splits[2], (BLOCK_TOTAL, VARIANT_COUNT), jnp.float32) ** block_scale(part_splits[2], (BLOCK_TOTAL, VARIANT_COUNT), ((0, 4),), -0.2, 0.2)), 163.84, 16384.0)
    lambda_grid = jnp.clip(jnp.exp(jax.random.uniform(arg_keys[3], (LAMBDA_GRID_SIZE,), jnp.float32, math.log(163.84), math.log(16384.0))), 163.84, 16384.0)
    trait_levels = gaussian(part_splits[4], (SAMPLE_TOTAL, PROTEIN_COUNT), 1.0, 6.0, ((0, 32), (1, 2)))
    partition_labels = plant(jax.random.randint(arg_keys[5], (SAMPLE_TOTAL,), 0, FOLDS), jax.random.fold_in(arg_keys[5], 1), 0, FOLDS - 1).astype(jnp.int32)
    preceding_fits = gaussian(part_splits[6], (2, SAMPLE_TOTAL, EARLIER), 1.0, 6.0, ((0, 2), (1, 32), (2, 4)))
    return {"allele_matrix": allele_matrix, "orthonormal_frames": orthonormal_frames, "segment_variances": segment_variances, "lambda_grid": lambda_grid, "trait_levels": trait_levels, "partition_labels": partition_labels, "preceding_fits": preceding_fits}


def segment_fitted_trait(projected_traits, pairwise_inner, spectral_line, lambda_grid, partition_mask_real):
    remainder = jnp.sum(pairwise_inner, axis=1, keepdims=True) - pairwise_inner
    damping_ratio = 1.0 / (spectral_line[:, None] + lambda_grid[None, :])
    ridge_coefficients = (remainder[:, :, None, :] * damping_ratio[:, None, :, None]).astype(jnp.bfloat16)
    samples_number = projected_traits.shape[0]
    running_total = jnp.zeros((samples_number, LAMBDA_GRID_SIZE * PROTEIN_COUNT), jnp.float32)
    for holdout_index in range(FOLDS):
        lookup_table = ridge_coefficients[:, holdout_index].reshape(VARIANT_COUNT, LAMBDA_GRID_SIZE * PROTEIN_COUNT)
        running_total = running_total + partition_mask_real[:, holdout_index:holdout_index + 1] * jnp.dot(projected_traits, lookup_table, preferred_element_type=jnp.float32)
    return running_total.reshape(samples_number, LAMBDA_GRID_SIZE, PROTEIN_COUNT).astype(jnp.bfloat16)


def reference(allele_matrix, orthonormal_frames, segment_variances, lambda_grid, trait_levels, partition_labels, preceding_fits):
    member = partition_labels[:, None] == jnp.arange(FOLDS, dtype=jnp.int32)[None, :]
    partition_mask_real = member.astype(jnp.float32)
    masked = (member.astype(jnp.bfloat16)[:, :, None] * trait_levels[:, None, :]).reshape(SAMPLE_TOTAL, FOLDS * PROTEIN_COUNT)

    def one_block(entry_offset):
        start = (entry_offset * VARIANT_COUNT).astype(jnp.int32)
        genotype_cols = lax.dynamic_slice_in_dim(allele_matrix, start, VARIANT_COUNT, 1)
        projected_traits = jnp.dot(genotype_cols, orthonormal_frames[entry_offset], preferred_element_type=jnp.float32).astype(jnp.bfloat16)
        pairwise_inner = jnp.dot(projected_traits.T, masked, preferred_element_type=jnp.float32).reshape(VARIANT_COUNT, FOLDS, PROTEIN_COUNT)
        return segment_fitted_trait(projected_traits, pairwise_inner, segment_variances[entry_offset], lambda_grid, partition_mask_real)

    stacked = lax.map(one_block, jnp.arange(BLOCK_TOTAL, dtype=jnp.int32))
    level0_predictions = jnp.transpose(stacked, (1, 0, 2, 3))
    half_width = PROTEIN_COUNT // 2
    olds, crosses, news, fit_olds, fit_news = [], [], [], [], []
    for choice_index in range(2):
        column_slot = choice_index * half_width
        added_columns = level0_predictions[:, :, :, column_slot].reshape(SAMPLE_TOTAL, BLOCK_TOTAL * LAMBDA_GRID_SIZE)
        target = trait_levels[:, column_slot:column_slot + 1]
        old_cols = preceding_fits[choice_index]
        olds.append(jnp.dot(old_cols.T, old_cols, preferred_element_type=jnp.float32) / SAMPLE_TOTAL)
        crosses.append(jnp.dot(added_columns.T, old_cols, preferred_element_type=jnp.float32) / SAMPLE_TOTAL)
        news.append(jnp.dot(added_columns.T, added_columns, preferred_element_type=jnp.float32) / SAMPLE_TOTAL)
        fit_olds.append(jnp.dot(old_cols.T, target, preferred_element_type=jnp.float32)[:, 0] / SAMPLE_TOTAL)
        fit_news.append(jnp.dot(added_columns.T, target, preferred_element_type=jnp.float32)[:, 0] / SAMPLE_TOTAL)
    return (level0_predictions, jnp.stack(olds), jnp.stack(crosses), jnp.stack(news), jnp.stack(fit_olds), jnp.stack(fit_news))
```

```python
import jax
import jax.numpy as jnp
from jax import lax
from jax.sharding import Mesh, PartitionSpec as P


FOLDS = 4
NEAR = 4
LANES = 128

BF = jnp.bfloat16
F32 = jnp.float32


def exchange(blocks, axis):
    return lax.all_to_all(blocks, axis, split_axis=0, concat_axis=0, tiled=True)


def copies(block, count):
    return jnp.broadcast_to(block[None], (count, *block.shape))


def dot(left, right, dims):
    return lax.dot_general(left, right, (dims, ((), ())), preferred_element_type=F32)


def total(blocks):
    return jnp.sum(blocks.astype(F32), axis=0)


def per_device(
    allele_matrix,
    orthonormal_frames,
    segment_variances,
    lambda_grid,
    trait_levels,
    partition_labels,
    preceding_fits,
):
    row_count = allele_matrix.shape[0]
    block_count, var_width = orthonormal_frames.shape[:2]
    prot_width = trait_levels.shape[1]
    grid_size = lambda_grid.shape[0]
    near, far, blocks = (lax.axis_size(n) for n in ("near", "far", "blk"))
    samples = ("far", "near")
    inverse = 1.0 / float(row_count * near * far)

    old_cols = preceding_fits[0]
    old_all = exchange(copies(old_cols, blocks), "blk")
    rotated = [
        jnp.dot(
            allele_matrix[:, b * var_width : (b + 1) * var_width],
            orthonormal_frames[b],
            preferred_element_type=F32,
        ).astype(BF)
        for b in range(block_count)
    ]
    member = jnp.arange(FOLDS, dtype=jnp.int32)[:, None] == partition_labels[None, :]
    mask = member.astype(F32)
    traits = trait_levels.T
    masked = member.astype(BF)[:, None, :] * traits[None, :, :]
    masked_all = masked.reshape(FOLDS * prot_width, row_count)
    local = jnp.stack([dot(masked_all, r, ((1,), (0,))).astype(BF) for r in rotated])
    local_q = jnp.stack([dot(masked[:, 0], r, ((1,), (0,))).astype(BF) for r in rotated])

    old_width = old_cols.shape[1]
    share = blocks * old_width // (near * far)
    gram_local = jnp.concatenate(
        [dot(old_all[i], old_cols, ((0,), (0,))).astype(BF) for i in range(blocks)]
    )
    gram_local = gram_local.reshape(far, near, share, old_width)
    gram_local = jnp.moveaxis(gram_local, 1, 0).reshape(near, far * share, old_width)
    gram_near = lax.psum_scatter(gram_local, "near", scatter_dimension=0, tiled=True)
    gram_near = gram_near.reshape(far, share, old_width)
    gram_old = lax.psum_scatter(gram_near, "far", scatter_dimension=0, tiled=True)
    gram_old = gram_old.reshape(share, old_width).T.astype(F32) * inverse

    bulk = local.size // (near * LANES)
    slim = local_q.size // (near * LANES)
    packed = jnp.concatenate(
        [local.reshape(near, bulk, LANES), local_q.reshape(near, slim, LANES)], axis=1
    )
    near_sum = total(exchange(packed, "near")).astype(BF)
    packed = jnp.concatenate(
        [near_sum[:bulk].reshape(far, bulk // far, LANES), copies(near_sum[bulk:], far)], axis=1
    )
    packed = exchange(packed, "far")
    far_sum = total(packed)
    bulk_sum = far_sum[: bulk // far].astype(BF)

    damping = 1.0 / (segment_variances[:, None, :] + lambda_grid[None, :, None])
    slim_all = lax.all_gather(far_sum[bulk // far :], "near", axis=0, tiled=True)
    crossed_q = slim_all.reshape(block_count, FOLDS, var_width)
    remainder_q = jnp.sum(crossed_q, axis=1, keepdims=True) - crossed_q
    coeffs_q = (remainder_q[:, :, None, :] * damping[:, None, :, :]).astype(BF)
    coeffs_q = coeffs_q.reshape(block_count, FOLDS * grid_size, var_width)
    fits_q = [
        dot(coeffs_q[b], rotated[b], ((1,), (1,))).reshape(FOLDS, grid_size, row_count)
        for b in range(block_count)
    ]
    added = jnp.concatenate([jnp.sum(mask[:, None, :] * f, axis=0) for f in fits_q], axis=0)
    added = added.astype(BF)
    new_width = added.shape[0]
    new_all = exchange(copies(added, blocks), "blk").reshape(blocks * new_width, row_count)
    target = traits[:1]
    small = dot(added, jnp.concatenate([new_all, target], axis=0), ((1,), (1,)))
    left = jnp.concatenate([added, target], axis=0)
    cross = jnp.concatenate(
        [dot(left, old_all[i], ((1,), (0,))) for i in range(blocks)], axis=1
    )
    cross = jnp.moveaxis(cross.reshape(new_width + 1, near * far, share), 1, 0)
    cross = cross.reshape(near * far, (new_width + 1) * share)
    final = jnp.concatenate([cross, copies(small.reshape(-1), near * far)], axis=1)
    width = final.shape[1]
    final = jnp.pad(final, ((0, 0), (0, -width % LANES)))
    final = exchange(final, samples)
    final = jnp.sum(final, axis=0) * inverse
    cut = (new_width + 1) * share
    cross_sum = final[:cut].reshape(new_width + 1, share)
    small_sum = final[cut:width].reshape(new_width, blocks * new_width + 1)

    bulk_far = lax.all_gather(bulk_sum, "far", axis=0, tiled=True)
    bulk_all = lax.all_gather(bulk_far, "near", axis=0, tiled=True)
    crossed = bulk_all.reshape(block_count, FOLDS, prot_width, var_width).astype(F32)
    remainder = jnp.sum(crossed, axis=1, keepdims=True) - crossed
    preds = []
    for b in range(block_count):
        running = jnp.zeros((grid_size * prot_width, row_count), F32)
        for k in range(FOLDS):
            coeffs = (remainder[b, k][None] * damping[b][:, None, :]).astype(BF)
            coeffs = coeffs.reshape(grid_size * prot_width, var_width)
            running = running + mask[k][None] * dot(coeffs, rotated[b], ((1,), (1,)))
        preds.append(running.astype(BF).reshape(grid_size, prot_width, row_count))
    level0 = jnp.moveaxis(jnp.stack(preds), 3, 0)
    return (
        level0,
        gram_old[None],
        cross_sum[None, :new_width],
        small_sum[None, :, :-1],
        cross_sum[new_width:],
        small_sum[None, :, -1],
    )


def solution(mesh):
    grp, smp, blk, pen = (mesh.shape[n] for n in ("grp", "smp", "blk", "pen"))
    split = Mesh(
        mesh.devices.reshape(grp, smp // NEAR, NEAR, blk, pen),
        ("grp", "far", "near", "blk", "pen"),
    )
    smp = ("far", "near")
    placed = (
        P(smp, ("grp", "blk")),
        P(("grp", "blk"), None, None),
        P(("grp", "blk"), None),
        P(),
        P(smp, ("grp", "pen")),
        P(smp),
        P(("grp", "pen"), smp, "blk"),
    )
    return jax.shard_map(
        per_device,
        mesh=split,
        in_specs=placed,
        out_specs=(
            P(smp, ("grp", "blk"), None, "pen"),
            P(("grp", "pen"), "blk", smp),
            P(("grp", "pen"), "blk", smp),
            P(("grp", "pen"), "blk", None),
            P(("grp", "pen"), smp),
            P(("grp", "pen"), "blk"),
        ),
        check_vma=False,
    )
```

```python
import jax
import jax.numpy as jnp
from jax import lax
from jax.experimental import pallas as pl
from jax.experimental.pallas import tpu as pltpu
from jax.sharding import Mesh, PartitionSpec as P


FOLDS = 4
NEAR = 4
LANES = 128

BF = jnp.bfloat16
F32 = jnp.float32
ROWS = (((0,), (0,)), ((), ()))


def exchange(blocks, axis):
    return lax.all_to_all(blocks, axis, split_axis=0, concat_axis=0, tiled=True)


def copies(block, count):
    return jnp.broadcast_to(block[None], (count, *block.shape))


def dot(left, right, dims):
    return lax.dot_general(left, right, (dims, ((), ())), preferred_element_type=F32)


def total(blocks):
    return jnp.sum(blocks.astype(F32), axis=0)


def paired_gram(side, old_all, old_cols, near, share):
    blocks, row_count, width = old_all.shape
    runs = width // (near * share)
    half = near // 2

    def kernel(side_ref, one_ref, own_ref, gone_ref, kept_ref):
        gram = lax.dot_general(
            one_ref[0], own_ref[...], ROWS, preferred_element_type=F32
        ).astype(BF)
        first = side_ref[0] == 0
        for run in range(runs):
            for high in range(half):
                at = (run * near + 2 * high) * share
                even = gram[at : at + share]
                odd = gram[at + share : at + 2 * share]
                gone_ref[high, run] = jnp.where(first, odd, even)
                kept_ref[high, run] = jnp.where(first, even, odd)

    half_shape = jax.ShapeDtypeStruct((half, blocks * runs, share, width), BF)
    half_spec = pl.BlockSpec((half, runs, share, width), lambda j: (0, j, 0, 0))
    return pl.pallas_call(
        kernel,
        grid=(blocks,),
        in_specs=[
            pl.BlockSpec(memory_space=pltpu.SMEM),
            pl.BlockSpec((1, row_count, width), lambda j: (j, 0, 0)),
            pl.BlockSpec((row_count, width), lambda j: (0, 0)),
        ],
        out_specs=[half_spec, half_spec],
        out_shape=[half_shape, half_shape],
        name="paired_gram",
    )(side.astype(jnp.int32)[None], old_all, old_cols)


def per_device(
    allele_matrix,
    orthonormal_frames,
    segment_variances,
    lambda_grid,
    trait_levels,
    partition_labels,
    preceding_fits,
):
    row_count = allele_matrix.shape[0]
    block_count, var_width = orthonormal_frames.shape[:2]
    prot_width = trait_levels.shape[1]
    grid_size = lambda_grid.shape[0]
    near, far, blocks = (lax.axis_size(n) for n in ("near", "far", "blk"))
    inverse = 1.0 / float(row_count * near * far)

    old_cols = preceding_fits[0]
    old_width = old_cols.shape[1]
    share = blocks * old_width // (near * far)
    old_all = lax.all_gather(old_cols, "blk", axis=0)
    rotated = [
        jnp.dot(
            allele_matrix[:, b * var_width : (b + 1) * var_width],
            orthonormal_frames[b],
            preferred_element_type=F32,
        ).astype(BF)
        for b in range(block_count)
    ]
    member = jnp.arange(FOLDS, dtype=jnp.int32)[:, None] == partition_labels[None, :]
    mask = member.astype(F32)
    traits = trait_levels.T
    masked = member.astype(BF)[:, None, :] * traits[None, :, :]
    masked_all = masked.reshape(FOLDS * prot_width, row_count)
    local = jnp.stack([dot(masked_all, r, ((1,), (0,))).astype(BF) for r in rotated])
    local_q = jnp.stack([dot(masked[:, 0], r, ((1,), (0,))).astype(BF) for r in rotated])

    seat = lax.axis_index("near").astype(jnp.uint32)
    low, high = seat & jnp.uint32(1), seat >> jnp.uint32(1)
    gone, kept = paired_gram(low, old_all, old_cols, near, share)
    met = lax.ppermute(gone, "near", [(i, i ^ 1) for i in range(near)])
    halves = (kept.astype(F32) + met.astype(F32)).astype(BF)
    gone = lax.dynamic_index_in_dim(halves, high ^ jnp.uint32(1), 0, keepdims=False)
    met = lax.ppermute(gone, "near", [(i, i ^ 2) for i in range(near)])
    kept = lax.dynamic_index_in_dim(halves, high, 0, keepdims=False)
    gram_local = (kept.astype(F32) + met.astype(F32)).astype(BF)
    gram_old = lax.psum_scatter(gram_local, "far", scatter_dimension=0, tiled=True)
    gram_old = gram_old.reshape(share, old_width).T.astype(F32) * inverse

    bulk = block_count * FOLDS * prot_width // near
    slim = block_count * FOLDS
    packed = jnp.concatenate(
        [
            local.reshape(near, bulk, var_width),
            copies(local_q.reshape(slim, var_width), near),
        ],
        axis=1,
    )
    packed = exchange(packed, "near")
    near_sum = total(packed).astype(BF)
    packed = jnp.concatenate(
        [near_sum[:bulk].reshape(far, bulk // far, var_width), copies(near_sum[bulk:], far)],
        axis=1,
    )
    packed = exchange(packed, "far")
    far_sum = total(packed)
    bulk_sum = far_sum[: bulk // far].astype(BF)

    damping = 1.0 / (segment_variances[:, None, :] + lambda_grid[None, :, None])
    crossed_q = far_sum[bulk // far :].reshape(block_count, FOLDS, var_width)
    remainder_q = jnp.sum(crossed_q, axis=1, keepdims=True) - crossed_q
    coeffs_q = (remainder_q[:, :, None, :] * damping[:, None, :, :]).astype(BF)
    coeffs_q = coeffs_q.reshape(block_count, FOLDS * grid_size, var_width)
    fits_q = [
        dot(coeffs_q[b], rotated[b], ((1,), (1,))).reshape(FOLDS, grid_size, row_count)
        for b in range(block_count)
    ]
    added = jnp.concatenate([jnp.sum(mask[:, None, :] * f, axis=0) for f in fits_q], axis=0)
    added = added.astype(BF)
    new_width = added.shape[0]
    new_all = exchange(copies(added, blocks), "blk").reshape(blocks * new_width, row_count)
    target = traits[:1]
    small = dot(added, jnp.concatenate([new_all, target], axis=0), ((1,), (1,)))
    left = jnp.concatenate([added, target], axis=0)
    cross = jnp.stack([dot(left, old_all[i], ((1,), (0,))) for i in range(blocks)])
    cross = cross.reshape(blocks, new_width + 1, far // blocks, near, share)
    cross = jnp.transpose(cross, (3, 0, 2, 1, 4)).reshape(near, far * (new_width + 1) * share)
    sums = jnp.concatenate([cross, copies(small.reshape(-1), near)], axis=1)
    width = sums.shape[1]
    sums = jnp.pad(sums, ((0, 0), (0, -width % (8 * LANES)))).reshape(near, -1, LANES)
    sums = total(exchange(sums, "near")).reshape(-1)
    cut = (new_width + 1) * share
    sums = jnp.concatenate(
        [sums[: far * cut].reshape(far, cut), copies(sums[far * cut : width], far)], axis=1
    )
    width = sums.shape[1]
    sums = jnp.pad(sums, ((0, 0), (0, -width % (8 * LANES)))).reshape(far, -1, LANES)
    bulk_rows = bulk_sum.size // LANES
    packed = jnp.concatenate(
        [copies(bulk_sum.reshape(bulk_rows, LANES), far), sums.astype(BF)], axis=1
    )
    packed = exchange(packed, "far")
    bulk_far = packed[:, :bulk_rows].reshape(bulk, var_width)
    bulk_all = exchange(copies(bulk_far, near), "near")
    final = (total(packed[:, bulk_rows:]) * inverse).reshape(-1)
    cross_sum = final[:cut].reshape(new_width + 1, share)
    small_sum = final[cut:width].reshape(new_width, blocks * new_width + 1)
    crossed = bulk_all.reshape(block_count, FOLDS, prot_width, var_width).astype(F32)
    remainder = jnp.sum(crossed, axis=1, keepdims=True) - crossed
    preds = []
    for b in range(block_count):
        running = jnp.zeros((grid_size * prot_width, row_count), F32)
        for k in range(FOLDS):
            coeffs = (remainder[b, k][None] * damping[b][:, None, :]).astype(BF)
            coeffs = coeffs.reshape(grid_size * prot_width, var_width)
            running = running + mask[k][None] * dot(coeffs, rotated[b], ((1,), (1,)))
        preds.append(running.astype(BF).reshape(grid_size, prot_width, row_count))
    level0 = jnp.moveaxis(jnp.stack(preds), 3, 0)
    return (
        level0,
        gram_old[None],
        cross_sum[None, :new_width],
        small_sum[None, :, :-1],
        cross_sum[new_width:],
        small_sum[None, :, -1],
    )


def solution(mesh):
    grp, smp, blk, pen = (mesh.shape[n] for n in ("grp", "smp", "blk", "pen"))
    split = Mesh(
        mesh.devices.reshape(grp, smp // NEAR, NEAR, blk, pen),
        ("grp", "far", "near", "blk", "pen"),
    )
    smp = ("far", "near")
    placed = (
        P(smp, ("grp", "blk")),
        P(("grp", "blk"), None, None),
        P(("grp", "blk"), None),
        P(),
        P(smp, ("grp", "pen")),
        P(smp),
        P(("grp", "pen"), smp, "blk"),
    )
    return jax.shard_map(
        per_device,
        mesh=split,
        in_specs=placed,
        out_specs=(
            P(smp, ("grp", "blk"), None, "pen"),
            P(("grp", "pen"), "blk", smp),
            P(("grp", "pen"), "blk", smp),
            P(("grp", "pen"), "blk", None),
            P(("grp", "pen"), smp),
            P(("grp", "pen"), "blk"),
        ),
        check_vma=False,
    )
```

```python
import jax
import jax.numpy as jnp
from jax import lax
from jax.experimental import pallas as pl
from jax.experimental.pallas import tpu as pltpu
from jax.sharding import Mesh, PartitionSpec as P


FOLDS = 4
NEAR = 4
LANES = 128

BF = jnp.bfloat16
F32 = jnp.float32
ROWS = (((0,), (0,)), ((), ()))


def exchange(blocks, axis):
    return lax.all_to_all(blocks, axis, split_axis=0, concat_axis=0, tiled=True)


def copies(block, count):
    return jnp.broadcast_to(block[None], (count, *block.shape))


def dot(left, right, dims):
    return lax.dot_general(left, right, (dims, ((), ())), preferred_element_type=F32)


def total(blocks):
    return jnp.sum(blocks.astype(F32), axis=0)


def paired_gram(side, spots, olds, near, share):
    _, width = olds[0].shape
    blocks = len(olds)
    runs = width // (near * share)
    half = near // 2

    def kernel(side_ref, spots_ref, *refs):
        own_ref, gone_ref, kept_ref = refs[0], refs[-2], refs[-1]
        first = side_ref[0] == 0
        for j in range(blocks):
            gram = lax.dot_general(
                refs[j][...], own_ref[...], ROWS, preferred_element_type=F32
            ).astype(BF)
            spot = spots_ref[j] * runs
            for run in range(runs):
                for high in range(half):
                    at = (run * near + 2 * high) * share
                    even = gram[at : at + share]
                    odd = gram[at + share : at + 2 * share]
                    gone_ref[high, spot + run] = jnp.where(first, odd, even)
                    kept_ref[high, spot + run] = jnp.where(first, even, odd)

    half_shape = jax.ShapeDtypeStruct((half, blocks * runs, share, width), BF)
    smem, vmem = pl.BlockSpec(memory_space=pltpu.SMEM), pl.BlockSpec(memory_space=pltpu.VMEM)
    return pl.pallas_call(
        kernel,
        in_specs=[smem, smem] + [vmem] * blocks,
        out_specs=[vmem, vmem],
        out_shape=[half_shape, half_shape],
        name="paired_gram",
    )(side.astype(jnp.int32)[None], spots.astype(jnp.int32), *olds)


def narrow(block):
    return jnp.concatenate(
        [block[..., i : i + LANES] for i in range(0, block.shape[-1], LANES)], axis=-2
    )


def widen(block, rows):
    return jnp.concatenate(
        [block[..., i : i + rows, :] for i in range(0, block.shape[-2], rows)], axis=-1
    )


def per_device(
    allele_matrix,
    orthonormal_frames,
    segment_variances,
    lambda_grid,
    trait_levels,
    partition_labels,
    preceding_fits,
):
    row_count = allele_matrix.shape[0]
    block_count, var_width = orthonormal_frames.shape[:2]
    prot_width = trait_levels.shape[1]
    grid_size = lambda_grid.shape[0]
    near, far, blocks = (lax.axis_size(n) for n in ("near", "far", "blk"))
    inverse = 1.0 / float(row_count * near * far)

    old_cols = preceding_fits[0]
    old_width = old_cols.shape[1]
    share = blocks * old_width // (near * far)
    place = lax.axis_index("blk").astype(jnp.uint32)
    shifts = (0, *sorted(range(1, blocks), key=lambda s: min(s, blocks - s)))
    olds = [
        lax.ppermute(old_cols, "blk", [(i, (i + s) % blocks) for i in range(blocks)])
        if s
        else old_cols
        for s in shifts
    ]
    back = jnp.array([blocks - s for s in shifts], jnp.uint32)
    spots = lax.rem(place + back, jnp.full((blocks,), blocks, jnp.uint32))
    rotated = [
        jnp.dot(
            allele_matrix[:, b * var_width : (b + 1) * var_width],
            orthonormal_frames[b],
            preferred_element_type=F32,
        ).astype(BF)
        for b in range(block_count)
    ]
    member = jnp.arange(FOLDS, dtype=jnp.int32)[:, None] == partition_labels[None, :]
    mask = member.astype(F32)
    traits = trait_levels.T
    masked = member.astype(BF)[:, None, :] * traits[None, :, :]
    masked_all = masked.reshape(FOLDS * prot_width, row_count)
    local = jnp.stack([dot(masked_all, r, ((1,), (0,))).astype(BF) for r in rotated])
    local_q = jnp.stack([dot(masked[:, 0], r, ((1,), (0,))).astype(BF) for r in rotated])

    seat = lax.axis_index("near").astype(jnp.uint32)
    low, high = seat & jnp.uint32(1), seat >> jnp.uint32(1)
    gone, kept = paired_gram(low, spots, olds, near, share)
    met = lax.ppermute(gone, "near", [(i, i ^ 1) for i in range(near)])
    halves = (kept.astype(F32) + met.astype(F32)).astype(BF)
    gone = lax.dynamic_index_in_dim(halves, high ^ jnp.uint32(1), 0, keepdims=False)
    met = lax.ppermute(gone, "near", [(i, i ^ 2) for i in range(near)])
    kept = lax.dynamic_index_in_dim(halves, high, 0, keepdims=False)
    gram_local = (kept.astype(F32) + met.astype(F32)).astype(BF)

    bulk = block_count * FOLDS * prot_width // near
    slim = block_count * FOLDS
    packed = jnp.concatenate(
        [
            local.reshape(near, bulk, var_width),
            copies(local_q.reshape(slim, var_width), near),
        ],
        axis=1,
    )
    packed = exchange(packed, "near")
    near_sum = total(packed).astype(BF)
    packed = jnp.concatenate(
        [near_sum[:bulk].reshape(far, bulk // far, var_width), copies(near_sum[bulk:], far)],
        axis=1,
    )
    packed = exchange(packed, "far")
    far_sum = total(packed)
    bulk_sum = far_sum[: bulk // far].astype(BF)

    damping = 1.0 / (segment_variances[:, None, :] + lambda_grid[None, :, None])
    crossed_q = far_sum[bulk // far :].reshape(block_count, FOLDS, var_width)
    remainder_q = jnp.sum(crossed_q, axis=1, keepdims=True) - crossed_q
    coeffs_q = (remainder_q[:, :, None, :] * damping[:, None, :, :]).astype(BF)
    coeffs_q = coeffs_q.reshape(block_count, FOLDS * grid_size, var_width)
    fits_q = [
        dot(coeffs_q[b], rotated[b], ((1,), (1,))).reshape(FOLDS, grid_size, row_count)
        for b in range(block_count)
    ]
    added = jnp.concatenate([jnp.sum(mask[:, None, :] * f, axis=0) for f in fits_q], axis=0)
    added = added.astype(BF)
    new_width = added.shape[0]
    new_all = exchange(copies(added, blocks), "blk").reshape(blocks * new_width, row_count)
    target = traits[:1]
    small = dot(added, jnp.concatenate([new_all, target], axis=0), ((1,), (1,)))
    left = jnp.concatenate([added, target], axis=0)
    turned = [olds[shifts.index(-m % blocks)] for m in range(blocks)]
    cross = jnp.stack([dot(left, old, ((1,), (0,))) for old in turned])
    cross = cross.reshape(blocks, new_width + 1, far // blocks, near, share)
    cross = jnp.transpose(cross, (3, 0, 2, 1, 4)).reshape(near, far * (new_width + 1) * share)
    sums = jnp.concatenate([cross, copies(small.reshape(-1), near)], axis=1)
    width = sums.shape[1]
    sums = jnp.pad(sums, ((0, 0), (0, -width % (8 * LANES)))).reshape(near, -1, LANES)
    sums = total(exchange(sums, "near")).reshape(-1)
    cut = (new_width + 1) * share
    cross = sums[: far * cut].astype(BF).reshape(blocks, far // blocks, cut)
    cross = lax.dynamic_slice_in_dim(
        jnp.concatenate([cross, cross]),
        lax.rem(jnp.uint32(blocks) - place, jnp.uint32(blocks)),
        blocks,
        0,
    )
    sums = jnp.concatenate(
        [cross.reshape(far, cut), copies(sums[far * cut : width].astype(BF), far)], axis=1
    )
    width = sums.shape[1]
    sums = jnp.pad(sums, ((0, 0), (0, -width % (8 * LANES)))).reshape(far, -1, LANES)
    slab = narrow(bulk_sum)
    packed = jnp.concatenate([copies(slab, far), sums, narrow(gram_local)], axis=1)
    mid = slab.shape[0] + sums.shape[1]
    packed = exchange(packed, "far")
    bulk_far = widen(packed[:, : slab.shape[0]], bulk_sum.shape[0]).reshape(bulk, var_width)
    bulk_all = exchange(copies(bulk_far, near), "near")
    final = (total(packed[:, slab.shape[0] : mid]) * inverse).reshape(-1)
    gram_old = widen(total(packed[:, mid:]), share).T * inverse
    cross_sum = final[:cut].reshape(new_width + 1, share)
    small_sum = final[cut:width].reshape(new_width, blocks * new_width + 1)
    crossed = bulk_all.reshape(block_count, FOLDS, prot_width, var_width).astype(F32)
    remainder = jnp.sum(crossed, axis=1, keepdims=True) - crossed
    preds = []
    for b in range(block_count):
        running = jnp.zeros((grid_size * prot_width, row_count), F32)
        for k in range(FOLDS):
            coeffs = (remainder[b, k][None] * damping[b][:, None, :]).astype(BF)
            coeffs = coeffs.reshape(grid_size * prot_width, var_width)
            running = running + mask[k][None] * dot(coeffs, rotated[b], ((1,), (1,)))
        preds.append(running.astype(BF).reshape(grid_size, prot_width, row_count))
    level0 = jnp.moveaxis(jnp.stack(preds), 3, 0)
    return (
        level0,
        gram_old[None],
        cross_sum[None, :new_width],
        small_sum[None, :, :-1],
        cross_sum[new_width:],
        small_sum[None, :, -1],
    )


def solution(mesh):
    grp, smp, blk, pen = (mesh.shape[n] for n in ("grp", "smp", "blk", "pen"))
    split = Mesh(
        mesh.devices.reshape(grp, smp // NEAR, NEAR, blk, pen),
        ("grp", "far", "near", "blk", "pen"),
    )
    smp = ("far", "near")
    placed = (
        P(smp, ("grp", "blk")),
        P(("grp", "blk"), None, None),
        P(("grp", "blk"), None),
        P(),
        P(smp, ("grp", "pen")),
        P(smp),
        P(("grp", "pen"), smp, "blk"),
    )
    return jax.shard_map(
        per_device,
        mesh=split,
        in_specs=placed,
        out_specs=(
            P(smp, ("grp", "blk"), None, "pen"),
            P(("grp", "pen"), "blk", smp),
            P(("grp", "pen"), "blk", smp),
            P(("grp", "pen"), "blk", None),
            P(("grp", "pen"), smp),
            P(("grp", "pen"), "blk"),
        ),
        check_vma=False,
    )
```

```python
import jax
import jax.numpy as jnp
from jax import lax
from jax.experimental import pallas as pl
from jax.experimental.pallas import tpu as pltpu
from jax.sharding import Mesh, PartitionSpec as P


FOLDS = 4
NEAR = 4
LANES = 128

BF = jnp.bfloat16
F32 = jnp.float32
ROWS = (((0,), (0,)), ((), ()))


def exchange(blocks, axis):
    return lax.all_to_all(blocks, axis, split_axis=0, concat_axis=0, tiled=True)


def copies(block, count):
    return jnp.broadcast_to(block[None], (count, *block.shape))


def dot(left, right, dims):
    return lax.dot_general(left, right, (dims, ((), ())), preferred_element_type=F32)


def total(blocks):
    return jnp.sum(blocks.astype(F32), axis=0)


def paired_gram(side, spots, olds, near, share):
    _, width = olds[0].shape
    blocks = len(olds)
    runs = width // (near * share)
    half = near // 2

    def kernel(side_ref, spots_ref, *refs):
        own_ref, gone_ref, kept_ref = refs[0], refs[-2], refs[-1]
        first = side_ref[0] == 0
        for j in range(blocks):
            gram = lax.dot_general(
                refs[j][...], own_ref[...], ROWS, preferred_element_type=F32
            ).astype(BF)
            spot = spots_ref[j] * runs
            for run in range(runs):
                for high in range(half):
                    at = (run * near + 2 * high) * share
                    even = gram[at : at + share]
                    odd = gram[at + share : at + 2 * share]
                    gone_ref[high, spot + run] = jnp.where(first, odd, even)
                    kept_ref[high, spot + run] = jnp.where(first, even, odd)

    half_shape = jax.ShapeDtypeStruct((half, blocks * runs, share, width), BF)
    smem, vmem = pl.BlockSpec(memory_space=pltpu.SMEM), pl.BlockSpec(memory_space=pltpu.VMEM)
    return pl.pallas_call(
        kernel,
        in_specs=[smem, smem] + [vmem] * blocks,
        out_specs=[vmem, vmem],
        out_shape=[half_shape, half_shape],
        name="paired_gram",
    )(side.astype(jnp.int32)[None], spots.astype(jnp.int32), *olds)


def narrow(block):
    return jnp.concatenate(
        [block[..., i : i + LANES] for i in range(0, block.shape[-1], LANES)], axis=-2
    )


def widen(block, rows):
    return jnp.concatenate(
        [block[..., i : i + rows, :] for i in range(0, block.shape[-2], rows)], axis=-1
    )


def per_device(
    allele_matrix,
    orthonormal_frames,
    segment_variances,
    lambda_grid,
    trait_levels,
    partition_labels,
    preceding_fits,
):
    row_count = allele_matrix.shape[0]
    block_count, var_width = orthonormal_frames.shape[:2]
    prot_width = trait_levels.shape[1]
    grid_size = lambda_grid.shape[0]
    near, wide, blocks = (lax.axis_size(n) for n in ("near", "wide", "blk"))
    far = wide * lax.axis_size("mid")
    away = ("wide", "mid")
    inverse = 1.0 / float(row_count * near * far)

    old_cols = preceding_fits[0]
    old_width = old_cols.shape[1]
    share = blocks * old_width // (near * far)
    place = lax.axis_index("blk").astype(jnp.uint32)
    shifts = (0, *sorted(range(1, blocks), key=lambda s: min(s, blocks - s)))
    olds = [
        lax.ppermute(old_cols, "blk", [(i, (i + s) % blocks) for i in range(blocks)])
        if s
        else old_cols
        for s in shifts
    ]
    back = jnp.array([blocks - s for s in shifts], jnp.uint32)
    spots = lax.rem(place + back, jnp.full((blocks,), blocks, jnp.uint32))
    rotated = [
        jnp.dot(
            allele_matrix[:, b * var_width : (b + 1) * var_width],
            orthonormal_frames[b],
            preferred_element_type=F32,
        ).astype(BF)
        for b in range(block_count)
    ]
    member = jnp.arange(FOLDS, dtype=jnp.int32)[:, None] == partition_labels[None, :]
    mask = member.astype(F32)
    traits = trait_levels.T
    masked = member.astype(BF)[:, None, :] * traits[None, :, :]
    masked_all = masked.reshape(FOLDS * prot_width, row_count)
    local = jnp.stack([dot(masked_all, r, ((1,), (0,))).astype(BF) for r in rotated])
    local_q = jnp.stack([dot(masked[:, 0], r, ((1,), (0,))).astype(BF) for r in rotated])

    seat = lax.axis_index("near").astype(jnp.uint32)
    low, high = seat & jnp.uint32(1), seat >> jnp.uint32(1)
    gone, kept = paired_gram(low, spots, olds, near, share)
    met = lax.ppermute(gone, "near", [(i, i ^ 1) for i in range(near)])
    halves = (kept.astype(F32) + met.astype(F32)).astype(BF)
    gone = lax.dynamic_index_in_dim(halves, high ^ jnp.uint32(1), 0, keepdims=False)
    met = lax.ppermute(gone, "near", [(i, i ^ 2) for i in range(near)])
    kept = lax.dynamic_index_in_dim(halves, high, 0, keepdims=False)
    gram_local = (kept.astype(F32) + met.astype(F32)).astype(BF)

    part = lax.axis_index("mid").astype(jnp.uint32)
    gram_local = gram_local.reshape(wide, far // wide, share, old_width)
    gone = lax.dynamic_index_in_dim(gram_local, part ^ jnp.uint32(1), 1, keepdims=False)
    met = lax.ppermute(gone, "mid", [(0, 1), (1, 0)])
    kept = lax.dynamic_index_in_dim(gram_local, part, 1, keepdims=False)
    gram_local = (kept.astype(F32) + met.astype(F32)).astype(BF)

    bulk = block_count * FOLDS * prot_width // near
    slim = block_count * FOLDS
    packed = jnp.concatenate(
        [
            local.reshape(near, bulk, var_width),
            copies(local_q.reshape(slim, var_width), near),
        ],
        axis=1,
    )
    packed = exchange(packed, "near")
    near_sum = total(packed).astype(BF)
    packed = jnp.concatenate(
        [near_sum[:bulk].reshape(far, bulk // far, var_width), copies(near_sum[bulk:], far)],
        axis=1,
    )
    packed = exchange(packed, away)
    far_sum = total(packed)
    bulk_sum = far_sum[: bulk // far].astype(BF)

    damping = 1.0 / (segment_variances[:, None, :] + lambda_grid[None, :, None])
    crossed_q = far_sum[bulk // far :].reshape(block_count, FOLDS, var_width)
    remainder_q = jnp.sum(crossed_q, axis=1, keepdims=True) - crossed_q
    coeffs_q = (remainder_q[:, :, None, :] * damping[:, None, :, :]).astype(BF)
    coeffs_q = coeffs_q.reshape(block_count, FOLDS * grid_size, var_width)
    fits_q = [
        dot(coeffs_q[b], rotated[b], ((1,), (1,))).reshape(FOLDS, grid_size, row_count)
        for b in range(block_count)
    ]
    added = jnp.concatenate([jnp.sum(mask[:, None, :] * f, axis=0) for f in fits_q], axis=0)
    added = added.astype(BF)
    new_width = added.shape[0]
    new_all = exchange(copies(added, blocks), "blk").reshape(blocks * new_width, row_count)
    target = traits[:1]
    small = dot(added, jnp.concatenate([new_all, target], axis=0), ((1,), (1,)))
    left = jnp.concatenate([added, target], axis=0)
    turned = [olds[shifts.index(-m % blocks)] for m in range(blocks)]
    cross = jnp.stack([dot(left, old, ((1,), (0,))) for old in turned])
    cross = cross.reshape(blocks, new_width + 1, far // blocks, near, share)
    cross = jnp.transpose(cross, (3, 0, 2, 1, 4)).reshape(near, far * (new_width + 1) * share)
    sums = jnp.concatenate([cross, copies(small.reshape(-1), near)], axis=1)
    width = sums.shape[1]
    sums = jnp.pad(sums, ((0, 0), (0, -width % (8 * LANES)))).reshape(near, -1, LANES)
    sums = total(exchange(sums, "near")).reshape(-1)
    cut = (new_width + 1) * share
    cross = sums[: far * cut].astype(BF).reshape(blocks, far // blocks, cut)
    cross = lax.dynamic_slice_in_dim(
        jnp.concatenate([cross, cross]),
        lax.rem(jnp.uint32(blocks) - place, jnp.uint32(blocks)),
        blocks,
        0,
    )
    sums = jnp.concatenate(
        [cross.reshape(far, cut), copies(sums[far * cut : width].astype(BF), far)], axis=1
    )
    width = sums.shape[1]
    sums = jnp.pad(sums, ((0, 0), (0, -width % (8 * LANES)))).reshape(far, -1, LANES)
    slab = narrow(bulk_sum)
    packed = jnp.concatenate([copies(slab, far), sums], axis=1)
    packed = exchange(packed, away)
    bulk_far = widen(packed[:, : slab.shape[0]], bulk_sum.shape[0]).reshape(bulk, var_width)
    bulk_all = lax.all_gather(bulk_far, "near", axis=0, tiled=True)
    final = (total(packed[:, slab.shape[0] :]) * inverse).reshape(-1)
    gram_all = exchange(gram_local, "wide")
    gram_old = total(gram_all).T * inverse
    cross_sum = final[:cut].reshape(new_width + 1, share)
    small_sum = final[cut:width].reshape(new_width, blocks * new_width + 1)
    crossed = bulk_all.reshape(block_count, FOLDS, prot_width, var_width).astype(F32)
    remainder = jnp.sum(crossed, axis=1, keepdims=True) - crossed
    preds = []
    for b in range(block_count):
        running = jnp.zeros((grid_size * prot_width, row_count), F32)
        for k in range(FOLDS):
            coeffs = (remainder[b, k][None] * damping[b][:, None, :]).astype(BF)
            coeffs = coeffs.reshape(grid_size * prot_width, var_width)
            running = running + mask[k][None] * dot(coeffs, rotated[b], ((1,), (1,)))
        preds.append(running.astype(BF).reshape(grid_size, prot_width, row_count))
    level0 = jnp.moveaxis(jnp.stack(preds), 3, 0)
    return (
        level0,
        gram_old[None],
        cross_sum[None, :new_width],
        small_sum[None, :, :-1],
        cross_sum[new_width:],
        small_sum[None, :, -1],
    )


def solution(mesh):
    grp, smp, blk, pen = (mesh.shape[n] for n in ("grp", "smp", "blk", "pen"))
    split = Mesh(
        mesh.devices.reshape(grp, smp // (2 * NEAR), 2, NEAR, blk, pen),
        ("grp", "wide", "mid", "near", "blk", "pen"),
    )
    smp = ("wide", "mid", "near")
    placed = (
        P(smp, ("grp", "blk")),
        P(("grp", "blk"), None, None),
        P(("grp", "blk"), None),
        P(),
        P(smp, ("grp", "pen")),
        P(smp),
        P(("grp", "pen"), smp, "blk"),
    )
    return jax.shard_map(
        per_device,
        mesh=split,
        in_specs=placed,
        out_specs=(
            P(smp, ("grp", "blk"), None, "pen"),
            P(("grp", "pen"), "blk", smp),
            P(("grp", "pen"), "blk", smp),
            P(("grp", "pen"), "blk", None),
            P(("grp", "pen"), smp),
            P(("grp", "pen"), "blk"),
        ),
        check_vma=False,
    )
```

```python
import jax
import jax.numpy as jnp
from jax import lax
from jax.experimental import pallas as pl
from jax.experimental.pallas import tpu as pltpu
from jax.sharding import Mesh, PartitionSpec as P


FOLDS = 4
NEAR = 4
LANES = 128

BF = jnp.bfloat16
F32 = jnp.float32
ROWS = (((0,), (0,)), ((), ()))


def exchange(blocks, axis):
    return lax.all_to_all(blocks, axis, split_axis=0, concat_axis=0, tiled=True)


def copies(block, count):
    return jnp.broadcast_to(block[None], (count, *block.shape))


def dot(left, right, dims):
    return lax.dot_general(left, right, (dims, ((), ())), preferred_element_type=F32)


def total(blocks):
    return jnp.sum(blocks.astype(F32), axis=0)


def paired_gram(side, spots, olds, near, share):
    _, width = olds[0].shape
    blocks = len(olds)
    runs = width // (near * share)
    half = near // 2

    def kernel(side_ref, spots_ref, *refs):
        own_ref, gone_ref, kept_ref = refs[0], refs[-2], refs[-1]
        first = side_ref[0] == 0
        for j in range(blocks):
            gram = lax.dot_general(
                refs[j][...], own_ref[...], ROWS, preferred_element_type=F32
            ).astype(BF)
            spot = spots_ref[j] * runs
            for run in range(runs):
                for high in range(half):
                    at = (run * near + 2 * high) * share
                    even = gram[at : at + share]
                    odd = gram[at + share : at + 2 * share]
                    gone_ref[high, spot + run] = jnp.where(first, odd, even)
                    kept_ref[high, spot + run] = jnp.where(first, even, odd)

    half_shape = jax.ShapeDtypeStruct((half, blocks * runs, share, width), BF)
    smem, vmem = pl.BlockSpec(memory_space=pltpu.SMEM), pl.BlockSpec(memory_space=pltpu.VMEM)
    return pl.pallas_call(
        kernel,
        in_specs=[smem, smem] + [vmem] * blocks,
        out_specs=[vmem, vmem],
        out_shape=[half_shape, half_shape],
        name="paired_gram",
    )(side.astype(jnp.int32)[None], spots.astype(jnp.int32), *olds)


def narrow(block):
    return jnp.concatenate(
        [block[..., i : i + LANES] for i in range(0, block.shape[-1], LANES)], axis=-2
    )


def widen(block, rows):
    return jnp.concatenate(
        [block[..., i : i + rows, :] for i in range(0, block.shape[-2], rows)], axis=-1
    )


def per_device(
    allele_matrix,
    orthonormal_frames,
    segment_variances,
    lambda_grid,
    trait_levels,
    partition_labels,
    preceding_fits,
):
    row_count = allele_matrix.shape[0]
    block_count, var_width = orthonormal_frames.shape[:2]
    prot_width = trait_levels.shape[1]
    grid_size = lambda_grid.shape[0]
    near, wide, blocks = (lax.axis_size(n) for n in ("near", "wide", "blk"))
    far = wide * lax.axis_size("mid")
    away = ("wide", "mid")
    inverse = 1.0 / float(row_count * near * far)

    old_cols = preceding_fits[0]
    old_width = old_cols.shape[1]
    share = blocks * old_width // (near * far)
    place = lax.axis_index("blk").astype(jnp.uint32)
    shifts = (0, *sorted(range(1, blocks), key=lambda s: min(s, blocks - s)))
    olds = [
        lax.ppermute(old_cols, "blk", [(i, (i + s) % blocks) for i in range(blocks)])
        if s
        else old_cols
        for s in shifts
    ]
    back = jnp.array([blocks - s for s in shifts], jnp.uint32)
    spots = lax.rem(place + back, jnp.full((blocks,), blocks, jnp.uint32))
    rotated = [
        jnp.dot(
            allele_matrix[:, b * var_width : (b + 1) * var_width],
            orthonormal_frames[b],
            preferred_element_type=F32,
        ).astype(BF)
        for b in range(block_count)
    ]
    member = jnp.arange(FOLDS, dtype=jnp.int32)[:, None] == partition_labels[None, :]
    mask = member.astype(F32)
    traits = trait_levels.T
    masked = member.astype(BF)[:, None, :] * traits[None, :, :]
    masked_all = masked.reshape(FOLDS * prot_width, row_count)
    local = jnp.stack([dot(masked_all, r, ((1,), (0,))).astype(BF) for r in rotated])
    local_q = jnp.stack([dot(masked[:, 0], r, ((1,), (0,))).astype(BF) for r in rotated])

    seat = lax.axis_index("near").astype(jnp.uint32)
    low, high = seat & jnp.uint32(1), seat >> jnp.uint32(1)
    gone, kept = paired_gram(low, spots, olds, near, share)
    met = lax.ppermute(gone, "near", [(i, i ^ 1) for i in range(near)])
    halves = (kept.astype(F32) + met.astype(F32)).astype(BF)
    gone = lax.dynamic_index_in_dim(halves, high ^ jnp.uint32(1), 0, keepdims=False)
    met = lax.ppermute(gone, "near", [(i, i ^ 2) for i in range(near)])
    kept = lax.dynamic_index_in_dim(halves, high, 0, keepdims=False)
    gram_local = (kept.astype(F32) + met.astype(F32)).astype(BF)

    bulk = block_count * FOLDS * prot_width // near
    slim = block_count * FOLDS
    packed = jnp.concatenate(
        [
            local.reshape(near, bulk, var_width),
            copies(local_q.reshape(slim, var_width), near),
        ],
        axis=1,
    )
    packed = exchange(packed, "near")
    near_sum = total(packed).astype(BF)
    packed = jnp.concatenate(
        [near_sum[:bulk].reshape(far, bulk // far, var_width), copies(near_sum[bulk:], far)],
        axis=1,
    )
    packed = exchange(packed, away)
    far_sum = total(packed)
    bulk_sum = far_sum[: bulk // far].astype(BF)

    damping = 1.0 / (segment_variances[:, None, :] + lambda_grid[None, :, None])
    crossed_q = far_sum[bulk // far :].reshape(block_count, FOLDS, var_width)
    remainder_q = jnp.sum(crossed_q, axis=1, keepdims=True) - crossed_q
    coeffs_q = (remainder_q[:, :, None, :] * damping[:, None, :, :]).astype(BF)
    coeffs_q = coeffs_q.reshape(block_count, FOLDS * grid_size, var_width)
    fits_q = [
        dot(coeffs_q[b], rotated[b], ((1,), (1,))).reshape(FOLDS, grid_size, row_count)
        for b in range(block_count)
    ]
    added = jnp.concatenate([jnp.sum(mask[:, None, :] * f, axis=0) for f in fits_q], axis=0)
    added = added.astype(BF)
    new_width = added.shape[0]
    target = traits[:1]
    left = jnp.concatenate([added, target], axis=0)
    turned = [olds[shifts.index(-m % blocks)] for m in range(blocks)]
    cross = jnp.stack([dot(left, old, ((1,), (0,))) for old in turned])
    cross = cross.reshape(blocks, new_width + 1, far // blocks, near, share)
    cut = (new_width + 1) * share
    cross = jnp.transpose(cross, (3, 0, 2, 1, 4)).reshape(near, far * cut)
    fit = dot(added, target, ((1,), (1,))).reshape(1, new_width)
    sums = jnp.concatenate([cross, jnp.broadcast_to(fit, (near, new_width))], axis=1)
    sums = jnp.pad(sums, ((0, 0), (0, -sums.shape[1] % (8 * row_count))))
    sums = sums.astype(BF).reshape(near, -1, row_count)
    mixed = jnp.concatenate([copies(added, near), sums], axis=1)
    mixed = jnp.broadcast_to(mixed[:, None], (near, blocks, *mixed.shape[1:]))
    mixed = exchange(mixed.reshape(near * blocks, *mixed.shape[2:]), ("near", "blk"))
    mixed = mixed.reshape(near, blocks, *mixed.shape[1:])
    mine = lax.dynamic_index_in_dim(mixed, place, 1, keepdims=False)
    sums = total(mine[:, new_width:]).reshape(-1)
    small = sum(
        dot(
            mine[n, :new_width],
            mixed[n, :, :new_width].reshape(blocks * new_width, row_count),
            ((1,), (1,)),
        )
        for n in range(near)
    )
    fit = sums[far * cut : far * cut + new_width].reshape(new_width, 1)
    small = jnp.concatenate([small, fit], axis=1).reshape(-1).astype(BF)
    cross = sums[: far * cut].astype(BF).reshape(blocks, far // blocks, cut)
    cross = lax.dynamic_slice_in_dim(
        jnp.concatenate([cross, cross]),
        lax.rem(jnp.uint32(blocks) - place, jnp.uint32(blocks)),
        blocks,
        0,
    )
    sums = jnp.concatenate(
        [cross.reshape(far, cut), copies(small, far)], axis=1
    )
    width = sums.shape[1]
    sums = jnp.pad(sums, ((0, 0), (0, -width % (8 * LANES)))).reshape(far, -1, LANES)
    slab = narrow(bulk_sum)
    packed = jnp.concatenate([copies(slab, far), sums], axis=1)
    packed = exchange(packed, away)
    bulk_far = widen(packed[:, : slab.shape[0]], bulk_sum.shape[0]).reshape(bulk, var_width)
    bulk_all = lax.all_gather(bulk_far, "near", axis=0, tiled=True)
    final = (total(packed[:, slab.shape[0] :]) * inverse).reshape(-1)
    gram_all = exchange(gram_local, away)
    gram_old = total(gram_all).T * inverse
    cross_sum = final[:cut].reshape(new_width + 1, share)
    small_sum = final[cut:width].reshape(new_width, blocks * new_width + 1)
    crossed = bulk_all.reshape(block_count, FOLDS, prot_width, var_width).astype(F32)
    remainder = jnp.sum(crossed, axis=1, keepdims=True) - crossed
    preds = []
    for b in range(block_count):
        running = jnp.zeros((grid_size * prot_width, row_count), F32)
        for k in range(FOLDS):
            coeffs = (remainder[b, k][None] * damping[b][:, None, :]).astype(BF)
            coeffs = coeffs.reshape(grid_size * prot_width, var_width)
            running = running + mask[k][None] * dot(coeffs, rotated[b], ((1,), (1,)))
        preds.append(running.astype(BF).reshape(grid_size, prot_width, row_count))
    level0 = jnp.moveaxis(jnp.stack(preds), 3, 0)
    return (
        level0,
        gram_old[None],
        cross_sum[None, :new_width],
        small_sum[None, :, :-1],
        cross_sum[new_width:],
        small_sum[None, :, -1],
    )


def solution(mesh):
    grp, smp, blk, pen = (mesh.shape[n] for n in ("grp", "smp", "blk", "pen"))
    split = Mesh(
        mesh.devices.reshape(grp, smp // (2 * NEAR), 2, NEAR, blk, pen),
        ("grp", "wide", "mid", "near", "blk", "pen"),
    )
    smp = ("wide", "mid", "near")
    placed = (
        P(smp, ("grp", "blk")),
        P(("grp", "blk"), None, None),
        P(("grp", "blk"), None),
        P(),
        P(smp, ("grp", "pen")),
        P(smp),
        P(("grp", "pen"), smp, "blk"),
    )
    return jax.shard_map(
        per_device,
        mesh=split,
        in_specs=placed,
        out_specs=(
            P(smp, ("grp", "blk"), None, "pen"),
            P(("grp", "pen"), "blk", smp),
            P(("grp", "pen"), "blk", smp),
            P(("grp", "pen"), "blk", None),
            P(("grp", "pen"), smp),
            P(("grp", "pen"), "blk"),
        ),
        check_vma=False,
    )
```

```python
import jax
import jax.numpy as jnp
from jax import lax
from jax.experimental import pallas as pl
from jax.experimental.pallas import tpu as pltpu
from jax.sharding import Mesh, PartitionSpec as P


FOLDS = 4
NEAR = 4
LANES = 128

BF = jnp.bfloat16
F32 = jnp.float32
ROWS = (((0,), (0,)), ((), ()))


def exchange(blocks, axis):
    return lax.all_to_all(blocks, axis, split_axis=0, concat_axis=0, tiled=True)


def copies(block, count):
    return jnp.broadcast_to(block[None], (count, *block.shape))


def dot(left, right, dims):
    return lax.dot_general(left, right, (dims, ((), ())), preferred_element_type=F32)


def total(blocks):
    return jnp.sum(blocks.astype(F32), axis=0)


def paired_gram(side, spots, olds, near, share):
    _, width = olds[0].shape
    blocks = len(olds)
    runs = width // (near * share)
    half = near // 2

    def kernel(side_ref, spots_ref, *refs):
        own_ref, gone_ref, kept_ref = refs[0], refs[-2], refs[-1]
        first = side_ref[0] == 0
        for j in range(blocks):
            gram = lax.dot_general(
                refs[j][...], own_ref[...], ROWS, preferred_element_type=F32
            ).astype(BF)
            spot = spots_ref[j] * runs
            for run in range(runs):
                for high in range(half):
                    at = (run * near + 2 * high) * share
                    even = gram[at : at + share]
                    odd = gram[at + share : at + 2 * share]
                    gone_ref[high, spot + run] = jnp.where(first, odd, even)
                    kept_ref[high, spot + run] = jnp.where(first, even, odd)

    half_shape = jax.ShapeDtypeStruct((half, blocks * runs, share, width), BF)
    smem, vmem = pl.BlockSpec(memory_space=pltpu.SMEM), pl.BlockSpec(memory_space=pltpu.VMEM)
    return pl.pallas_call(
        kernel,
        in_specs=[smem, smem] + [vmem] * blocks,
        out_specs=[vmem, vmem],
        out_shape=[half_shape, half_shape],
        name="paired_gram",
    )(side.astype(jnp.int32)[None], spots.astype(jnp.int32), *olds)


def narrow(block):
    return jnp.concatenate(
        [block[..., i : i + LANES] for i in range(0, block.shape[-1], LANES)], axis=-2
    )


def widen(block, rows):
    return jnp.concatenate(
        [block[..., i : i + rows, :] for i in range(0, block.shape[-2], rows)], axis=-1
    )


def per_device(
    allele_matrix,
    orthonormal_frames,
    segment_variances,
    lambda_grid,
    trait_levels,
    partition_labels,
    preceding_fits,
):
    row_count = allele_matrix.shape[0]
    block_count, var_width = orthonormal_frames.shape[:2]
    prot_width = trait_levels.shape[1]
    grid_size = lambda_grid.shape[0]
    near, wide, blocks = (lax.axis_size(n) for n in ("near", "wide", "blk"))
    far = wide * lax.axis_size("mid")
    away = ("wide", "mid")
    inverse = 1.0 / float(row_count * near * far)

    old_cols = preceding_fits[0]
    old_width = old_cols.shape[1]
    share = blocks * old_width // (near * far)
    place = lax.axis_index("blk").astype(jnp.uint32)
    shifts = (0, *sorted(range(1, blocks), key=lambda s: min(s, blocks - s)))
    olds = [
        lax.ppermute(old_cols, "blk", [(i, (i + s) % blocks) for i in range(blocks)])
        if s
        else old_cols
        for s in shifts
    ]
    back = jnp.array([blocks - s for s in shifts], jnp.uint32)
    spots = lax.rem(place + back, jnp.full((blocks,), blocks, jnp.uint32))
    rotated = [
        jnp.dot(
            allele_matrix[:, b * var_width : (b + 1) * var_width],
            orthonormal_frames[b],
            preferred_element_type=F32,
        ).astype(BF)
        for b in range(block_count)
    ]
    member = jnp.arange(FOLDS, dtype=jnp.int32)[:, None] == partition_labels[None, :]
    mask = member.astype(F32)
    traits = trait_levels.T
    masked = member.astype(BF)[:, None, :] * traits[None, :, :]
    masked_all = masked.reshape(FOLDS * prot_width, row_count)
    local = jnp.stack([dot(masked_all, r, ((1,), (0,))).astype(BF) for r in rotated])
    local_q = jnp.stack([dot(masked[:, 0], r, ((1,), (0,))).astype(BF) for r in rotated])

    seat = lax.axis_index("near").astype(jnp.uint32)
    low, high = seat & jnp.uint32(1), seat >> jnp.uint32(1)
    gone, kept = paired_gram(low, spots, olds, near, share)
    met = lax.ppermute(gone, "near", [(i, i ^ 1) for i in range(near)])
    halves = (kept.astype(F32) + met.astype(F32)).astype(BF)
    gone = lax.dynamic_index_in_dim(halves, high ^ jnp.uint32(1), 0, keepdims=False)
    met = lax.ppermute(gone, "near", [(i, i ^ 2) for i in range(near)])
    kept = lax.dynamic_index_in_dim(halves, high, 0, keepdims=False)
    gram_local = (kept.astype(F32) + met.astype(F32)).astype(BF)

    bulk = block_count * FOLDS * prot_width // near
    slim = block_count * FOLDS
    packed = jnp.concatenate(
        [
            local.reshape(near, bulk, var_width),
            copies(local_q.reshape(slim, var_width), near),
        ],
        axis=1,
    )
    packed = exchange(packed, "near")
    near_sum = total(packed).astype(BF)
    packed = jnp.concatenate(
        [near_sum[:bulk].reshape(far, bulk // far, var_width), copies(near_sum[bulk:], far)],
        axis=1,
    )
    packed = exchange(packed, away)
    far_sum = total(packed)
    bulk_sum = far_sum[: bulk // far].astype(BF)

    damping = 1.0 / (segment_variances[:, None, :] + lambda_grid[None, :, None])
    crossed_q = far_sum[bulk // far :].reshape(block_count, FOLDS, var_width)
    remainder_q = jnp.sum(crossed_q, axis=1, keepdims=True) - crossed_q
    coeffs_q = (remainder_q[:, :, None, :] * damping[:, None, :, :]).astype(BF)
    coeffs_q = coeffs_q.reshape(block_count, FOLDS * grid_size, var_width)
    fits_q = [
        dot(coeffs_q[b], rotated[b], ((1,), (1,))).reshape(FOLDS, grid_size, row_count)
        for b in range(block_count)
    ]
    added = jnp.concatenate([jnp.sum(mask[:, None, :] * f, axis=0) for f in fits_q], axis=0)
    added = added.astype(BF)
    new_width = added.shape[0]
    target = traits[:1]
    left = jnp.concatenate([added, target], axis=0)
    turned = [olds[shifts.index(-m % blocks)] for m in range(blocks)]
    cross = jnp.stack([dot(left, old, ((1,), (0,))) for old in turned])
    cross = cross.reshape(blocks, new_width + 1, far // blocks, near, share)
    cut = (new_width + 1) * share
    cross = jnp.transpose(cross, (3, 0, 2, 1, 4)).reshape(near, far * cut)
    fit = dot(added, target, ((1,), (1,))).reshape(1, new_width)
    sums = jnp.concatenate([cross, jnp.broadcast_to(fit, (near, new_width))], axis=1)
    sums = jnp.pad(sums, ((0, 0), (0, -sums.shape[1] % (8 * row_count))))
    sums = sums.astype(BF).reshape(near, -1, row_count)
    mixed = jnp.concatenate([copies(added, near), sums], axis=1)
    mixed = jnp.broadcast_to(mixed[:, None], (near, blocks, *mixed.shape[1:]))
    mixed = exchange(mixed.reshape(near * blocks, *mixed.shape[2:]), ("near", "blk"))
    mixed = mixed.reshape(near, blocks, *mixed.shape[1:])
    mine = lax.dynamic_index_in_dim(mixed, place, 1, keepdims=False)
    sums = total(mine[:, new_width:]).reshape(-1)
    small = sum(
        dot(
            mine[n, :new_width],
            mixed[n, :, :new_width].reshape(blocks * new_width, row_count),
            ((1,), (1,)),
        )
        for n in range(near)
    )
    fit = sums[far * cut : far * cut + new_width].reshape(new_width, 1)
    small = jnp.concatenate([small, fit], axis=1).reshape(-1).astype(BF)
    cross = sums[: far * cut].astype(BF).reshape(blocks, far // blocks, cut)
    cross = lax.dynamic_slice_in_dim(
        jnp.concatenate([cross, cross]),
        lax.rem(jnp.uint32(blocks) - place, jnp.uint32(blocks)),
        blocks,
        0,
    )
    sums = jnp.concatenate(
        [cross.reshape(far, cut), copies(small, far)], axis=1
    )
    width = sums.shape[1]
    sums = jnp.pad(sums, ((0, 0), (0, -width % (8 * LANES)))).reshape(far, -1, LANES)
    mid = sums.shape[1]
    packed = jnp.concatenate([sums, narrow(gram_local)], axis=1)
    packed = exchange(packed, away)
    bulk_all = lax.all_gather(bulk_sum, (*away, "near"), axis=0)
    bulk_all = bulk_all.reshape(far, near, *bulk_sum.shape)
    bulk_all = jnp.moveaxis(bulk_all, 1, 0)
    final = (total(packed[:, :mid]) * inverse).reshape(-1)
    gram_old = widen(total(packed[:, mid:]), share).T * inverse
    cross_sum = final[:cut].reshape(new_width + 1, share)
    small_sum = final[cut:width].reshape(new_width, blocks * new_width + 1)
    crossed = bulk_all.reshape(block_count, FOLDS, prot_width, var_width).astype(F32)
    remainder = jnp.sum(crossed, axis=1, keepdims=True) - crossed
    preds = []
    for b in range(block_count):
        running = jnp.zeros((grid_size * prot_width, row_count), F32)
        for k in range(FOLDS):
            coeffs = (remainder[b, k][None] * damping[b][:, None, :]).astype(BF)
            coeffs = coeffs.reshape(grid_size * prot_width, var_width)
            running = running + mask[k][None] * dot(coeffs, rotated[b], ((1,), (1,)))
        preds.append(running.astype(BF).reshape(grid_size, prot_width, row_count))
    level0 = jnp.moveaxis(jnp.stack(preds), 3, 0)
    return (
        level0,
        gram_old[None],
        cross_sum[None, :new_width],
        small_sum[None, :, :-1],
        cross_sum[new_width:],
        small_sum[None, :, -1],
    )


def solution(mesh):
    grp, smp, blk, pen = (mesh.shape[n] for n in ("grp", "smp", "blk", "pen"))
    split = Mesh(
        mesh.devices.reshape(grp, smp // (2 * NEAR), 2, NEAR, blk, pen),
        ("grp", "wide", "mid", "near", "blk", "pen"),
    )
    smp = ("wide", "mid", "near")
    placed = (
        P(smp, ("grp", "blk")),
        P(("grp", "blk"), None, None),
        P(("grp", "blk"), None),
        P(),
        P(smp, ("grp", "pen")),
        P(smp),
        P(("grp", "pen"), smp, "blk"),
    )
    return jax.shard_map(
        per_device,
        mesh=split,
        in_specs=placed,
        out_specs=(
            P(smp, ("grp", "blk"), None, "pen"),
            P(("grp", "pen"), "blk", smp),
            P(("grp", "pen"), "blk", smp),
            P(("grp", "pen"), "blk", None),
            P(("grp", "pen"), smp),
            P(("grp", "pen"), "blk"),
        ),
        check_vma=False,
    )
```
